32 devices in a mesh: gx: 2 (over core), gy: 4 (over y, x), gz: 4 (over z).
Axes of the slice: x: 2, y: 2, z: 4, core: 2. Of those that a mesh axis runs over, the one named last changes fastest.
Arguments:
- quant_codes: int32 [64, 128, 512], P('gx', 'gy', 'gz'), may hold values from -1073741824 to 1073741824, as said below
- error_step: float32 [1], replicated, may hold values from 4e-09 to 1.5e-08
Outputs:
- decoded: float32 [64, 128, 512], P('gx', 'gy', 'gz')
The draws below stay inside these ranges and needn't reach their ends.
Inputs may be any that keep to these rules, and one draw needn't show every extreme that they name: quant_codes are the third differences (along the three dimensions, with zeros before the grid's first cells) of a field of integers between -134217728 and 134217728.
All inputs are finite; a program needn't handle non-finite values.
Results may differ from the reference program's by a relative error of at most 0.00002.
Values sent between devices are 32-bit elements; how exact they have to be, the bound alone decides.
A program may use at most 64 MiB of HBM per device.

```python
import math
import jax
import jax.numpy as jnp

QMAX = 134217728
NX = 64
NY = 128
NZ = 512


def draw_quant_codes(key, part):
    levels_grid = jax.random.randint(jax.random.fold_in(key, 11), (NX, NY, NZ), -QMAX, QMAX + 1, dtype=jnp.int32)
    first = levels_grid - jnp.pad(levels_grid, ((1, 0), (0, 0), (0, 0)))[:-1]
    second = first - jnp.pad(first, ((0, 0), (1, 0), (0, 0)))[:, :-1]
    third = second - jnp.pad(second, ((0, 0), (0, 0), (1, 0)))[:, :, :-1]
    return third.astype(jnp.int32)


def setup_inputs(seed: int = 0) -> dict:
    streams_of = jax.random.split(jax.random.key(seed), 3)
    quant_codes = draw_quant_codes(jax.random.fold_in(streams_of[2], 71), 0)
    error_step = jnp.clip(jnp.exp(jax.random.uniform(streams_of[1], (1,), jnp.float32, math.log(3.999999886872274e-09), math.log(1.4999999464748726e-08))), 3.999999886872274e-09, 1.4999999464748726e-08)
    return {"quant_codes": quant_codes, "error_step": error_step}


def reference(quant_codes, error_step):
    prefix = jnp.cumsum(quant_codes, axis=0, dtype=jnp.int32)
    prefix = jnp.cumsum(prefix, axis=1, dtype=jnp.int32)
    prefix = jnp.cumsum(prefix, axis=2, dtype=jnp.int32)
    recon = prefix.astype(jnp.float32) * error_step[0]
    padded = jnp.pad(recon, 1)
    neighbours = padded[2:, 1:-1, 1:-1] + padded[:-2, 1:-1, 1:-1]
    neighbours = neighbours + padded[1:-1, 2:, 1:-1] + padded[1:-1, :-2, 1:-1]
    neighbours = neighbours + padded[1:-1, 1:-1, 2:] + padded[1:-1, 1:-1, :-2]
    return recon + 0.5 * (neighbours / 6.0 - recon)
```

```python
import functools

import jax
import jax.numpy as jnp
from jax import lax
from jax.experimental import pallas as pl
from jax.experimental.pallas import tpu as pltpu
from jax.sharding import PartitionSpec as P

MESH = pl.DeviceIdType.MESH
I32 = jnp.int32
F32 = jnp.float32
SUB = 8


def iota(shape, dim):
    return lax.broadcasted_iota(I32, shape, dim)


def turn(x, by, dim):
    n = x.shape[dim]
    by = by % n
    if by == 0:
        return x
    if dim == 1 and n % 128 != 0:
        return jnp.concatenate([x[:, n - by :], x[:, : n - by]], 1)
    return pltpu.roll(x, by, dim)


def lane_scan(x):
    n = x.shape[1]
    tri = (iota((n, n), 0) <= iota((n, n), 1)).astype(F32)
    one, big = tri.astype(jnp.bfloat16), (tri * 256.0).astype(jnp.bfloat16)

    def times(part, m):
        return jnp.dot(part.astype(F32).astype(jnp.bfloat16), m, preferred_element_type=F32)

    low = times(x & 255, one) + times((x >> 8) & 255, big)
    high = times((x >> 16) & 255, one) + times(x >> 24, big)
    return low.astype(I32) + (high.astype(I32) << 16)


def row_scan(x):
    rows, n = x.shape
    s = iota((SUB, n), 0)
    out, carry = [], None
    for b in range(rows // SUB):
        v = x[b * SUB : (b + 1) * SUB]
        for d in (1, 2, 4):
            v = v + jnp.where(s >= d, pltpu.roll(v, d, 0), 0)
        if carry is not None:
            v = v + carry
        carry = jnp.broadcast_to(v[SUB - 1 : SUB], (SUB, n))
        out.append(v)
    return jnp.concatenate(out, 0) if len(out) > 1 else out[0]


def exchange(
    mesh_sizes, q_hbm, v_ref, eh_ref,
    q, scan, xs, xup, xdn, ys, yt, yup, ytup, hy, ht, ydn, ytdn,
    z0, z2, z1, zup0, zup2, zup1, d0, d2, d1, zdn0, zdn2, zdn1,
    rx, hx, ry, ryt, ax, hxc, by, hyc, za0, za2, za1,
    load_sem, xss, xrs, yss, yrs, ytss, ytrs, z0ss, z0rs, z2ss, z2rs, z1ss, z1rs, dss, drs,
):
    nx, ny, nz = mesh_sizes
    ni, nj, nk = q.shape
    nb = nj // SUB
    nl = ni * nb
    X, Y, Z = (lax.axis_index(a) for a in ("gx", "gy", "gz"))
    place = {"gx": X, "gy": Y, "gz": Z}
    size = {"gx": nx, "gy": ny, "gz": nz}
    last_x, last_y, last_z = X == nx - 1, Y == ny - 1, Z == nz - 1

    load = pltpu.make_async_copy(q_hbm, q, load_sem)
    load.start()
    barrier = pltpu.get_barrier_semaphore()
    for axis in ("gz", "gy", "gx"):
        for d in range(1, size[axis]):
            pl.semaphore_signal(
                barrier, inc=1, device_id={axis: lax.rem(place[axis] + d, size[axis])},
                device_id_type=MESH,
            )

    ends = []

    def up(axis, src, slots, ssem, rsem):
        for d in range(1, size[axis]):
            def copy(d=d):
                return pltpu.make_async_remote_copy(
                    src_ref=src, dst_ref=slots.at[d - 1], send_sem=ssem.at[d - 1],
                    recv_sem=rsem.at[d - 1], device_id={axis: place[axis] + d},
                    device_id_type=MESH,
                )

            here = place[axis] + d < size[axis]

            @pl.when(here)
            def _():
                copy().start()

            ends.append((here, copy))

    def up_sum(axis, src, slots, ssem, rsem, total):
        total[...] = jnp.zeros_like(total)
        for d in range(1, size[axis]):
            @pl.when(place[axis] >= d)
            def _():
                pltpu.make_async_remote_copy(
                    src_ref=src, dst_ref=slots.at[d - 1], send_sem=ssem.at[d - 1],
                    recv_sem=rsem.at[d - 1], device_id={axis: place[axis]},
                    device_id_type=MESH,
                ).wait_recv()
                total[...] += slots[d - 1]

    def down_copy(axis, src, dst, n):
        return pltpu.make_async_remote_copy(
            src_ref=src, dst_ref=dst, send_sem=dss.at[n], recv_sem=drs.at[n],
            device_id={axis: place[axis] - 1}, device_id_type=MESH,
        )

    def down(axis, src, dst, n):
        here = place[axis] > 0

        @pl.when(here)
        def _():
            down_copy(axis, src, dst, n).start()

        ends.append((here, lambda: down_copy(axis, src, dst, n)))

    def down_wait(axis, src, dst, n):
        @pl.when(place[axis] < size[axis] - 1)
        def _():
            down_copy(axis, src, dst, n).wait_recv()

        @pl.when(place[axis] == size[axis] - 1)
        def _():
            dst[...] = jnp.zeros_like(dst)

    lanes = iota((SUB, nl), 1)
    subs = iota((SUB, nl), 0)

    load.wait()
    total = q[0]
    for i in range(1, ni):
        total = total + q[i]
    xs[...] = total
    pl.semaphore_wait(barrier, nx + ny + nz - 3)
    up("gx", xs, xup, xss, xrs)
    down("gx", q.at[0], xdn, 0)

    for i in range(ni):
        ys[pl.ds(i, 1), :] = jnp.sum(q[i], axis=0, keepdims=True)
        hy[pl.ds(i, 1), :] = q[i, 0:1, :]
    up("gy", ys, yup, yss, yrs)
    down("gy", hy, ydn, 1)

    step = 8

    def scan_block(g, _):
        rows = pl.ds(g * step, step)
        part = q[rows].reshape(step * nj, nk)
        scan[rows] = lane_scan(part).reshape(step, nj, nk)
        return 0

    lax.fori_loop(0, ni // step, scan_block, 0)

    up_sum("gx", xs, xup, xss, xrs, rx)
    down_wait("gx", q.at[0], xdn, 0)
    rxv, hxv = rx[...], xdn[...]
    sk = iota((SUB, nk), 0)
    yt[...] = jnp.where(
        sk == 0, jnp.sum(rxv, axis=0, keepdims=True),
        jnp.where(sk == 1, jnp.sum(hxv, axis=0, keepdims=True), 0),
    )
    ht[...] = jnp.where(sk == 0, rxv[0:1], 0)
    up("gy", yt, ytup, ytss, ytrs)
    down("gy", ht, ytdn, 2)

    a0 = jnp.zeros((SUB, nl), I32)
    b0 = jnp.zeros((SUB, nl), I32)
    for i in range(ni):
        for b in range(nb):
            rows = slice(b * SUB, (b + 1) * SUB)
            here = lanes == i * nb + b
            a0 = jnp.where(here, scan[i, rows, nk - 1 : nk], a0)
            b0 = jnp.where(here, q[i, rows, 0:1], b0)
    z0[...] = a0
    d0[...] = b0
    up("gz", z0, zup0, z0ss, z0rs)
    down("gz", d0, zdn0, 3)
    lx = lane_scan(jnp.concatenate([rxv, hxv], 0))
    a2 = jnp.zeros((SUB, nl), I32)
    b2 = jnp.zeros((SUB, nl), I32)
    for b in range(2 * nb):
        rows = slice(b * SUB, (b + 1) * SUB)
        a2 = jnp.where(lanes == b, lx[rows, nk - 1 : nk], a2)
        if b < nb:
            b2 = jnp.where(lanes == b, rxv[rows, 0:1], b2)
    z2[...] = a2
    d2[...] = b2
    up("gz", z2, zup2, z2ss, z2rs)
    down("gz", d2, zdn2, 4)
    ax[...] = row_scan(lx[:nj])
    hxc[...] = row_scan(lx[nj:])

    def cumulate(i, before):
        new = before + row_scan(scan[i])
        scan[i] = new
        return new

    lax.fori_loop(0, ni, cumulate, jnp.zeros((nj, nk), I32))

    up_sum("gy", ys, yup, yss, yrs, ry)
    up_sum("gy", yt, ytup, ytss, ytrs, ryt)
    down_wait("gy", hy, ydn, 1)
    down_wait("gy", ht, ytdn, 2)
    ryv, rytv = ry[...], ryt[...]
    ly = lane_scan(jnp.concatenate([ryv, ydn[...], rytv, ytdn[...]], 0))
    lyl, lyh = ly[:ni], ly[ni : 2 * ni]
    lyt, lyht = ly[2 * ni : 2 * ni + SUB], ly[2 * ni + SUB :]
    mine = (iota((ni, nl), 1) // nb) == iota((ni, nl), 0)
    first = (iota((1, nl), 1) // nb) == 0

    def along(column, extra):
        row = jnp.sum(jnp.where(mine, column, 0), axis=0, keepdims=True)
        return row + jnp.where(first, extra, 0)

    end = slice(nk - 1, nk)
    z1[...] = jnp.where(
        subs == 0, along(lyl[:, end], lyt[0:1, end]),
        jnp.where(
            subs == 1, along(lyh[:, end], lyht[0:1, end]),
            jnp.where(
                subs == 2, lyt[0:1, end], jnp.where(subs == 3, lyt[1:2, end], 0)
            ),
        ),
    )
    d1[...] = jnp.where(subs == 0, along(ryv[:, 0:1], rytv[0:1, 0:1]), 0)
    up("gz", z1, zup1, z1ss, z1rs)
    down("gz", d1, zdn1, 5)

    rows_i = iota((ni, nk), 0)
    by[...] = row_scan(lyl + jnp.where(rows_i == 0, lyt[0:1], 0))
    hyc[...] = row_scan(lyh + jnp.where(rows_i == 0, lyht[0:1], 0))
    jrow = iota((nj, nk), 0)
    klane = iota((nj, nk), 1)
    plane = ax[...]

    def field(i):
        return scan[i] + plane + by[pl.ds(i, 1), :]

    def stencil(i, low, mid, high):
        down_j = jnp.where(jrow == 0, by[pl.ds(i, 1), :], turn(mid, 1, 0))
        edge_j = jnp.where(last_y, 0, mid + hyc[pl.ds(i, 1), :])
        up_j = jnp.where(jrow == nj - 1, edge_j, turn(mid, nj - 1, 0))
        down_k = jnp.where(klane == 0, 0, turn(mid, 1, 1))
        edge_k = jnp.where(last_z, 0, mid)
        up_k = jnp.where(klane == nk - 1, edge_k, turn(mid, nk - 1, 1))
        v_ref[i] = 6 * mid + (low + high) + (down_j + up_j) + (down_k + up_k)

    def sweep(i, state):
        low, mid = state
        high = field(i + 1)
        stencil(i, low, mid, high)
        return mid, high

    low, mid = lax.fori_loop(0, ni - 1, sweep, (plane + lyt[0:1], field(0)))
    stencil(ni - 1, low, mid, jnp.where(last_x, 0, mid + hxc[...] + lyt[1:2]))

    up_sum("gz", z0, zup0, z0ss, z0rs, za0)
    up_sum("gz", z2, zup2, z2ss, z2rs, za2)
    down_wait("gz", d0, zdn0, 3)
    down_wait("gz", d2, zdn2, 4)
    up_sum("gz", z1, zup1, z1ss, z1rs, za1)
    down_wait("gz", d1, zdn1, 5)
    block = lax.rem(lanes, nb)

    def j_scan(w):
        for d in (1, 2, 4):
            w = w + jnp.where(subs >= d, pltpu.roll(w, d, 0), 0)
        whole = jnp.broadcast_to(w[SUB - 1 : SUB], w.shape)
        for d in range(1, nb):
            w = w + jnp.where(block >= d, turn(whole, d, 1), 0)
        return w

    def i_scan(w):
        d = nb
        while d < nl:
            w = w + jnp.where(lanes >= d, turn(w, d, 1), 0)
            d *= 2
        return w

    r2, r1 = za2[...], za1[...]
    y = i_scan(r1)
    y_low, y_high = y[0:1], y[1:2]
    corner, corner_high = r1[2:3], r1[3:4]
    D = i_scan(j_scan(za0[...] + jnp.where(lanes < nb, r2, 0))) + y_low
    xe = j_scan(r2)
    down_i = jnp.where(lanes < nb, xe + corner, turn(D, nb, 1))
    edge_i = jnp.where(last_x, 0, D + turn(xe, nl - 2 * nb, 1) + corner_high)
    up_i = jnp.where(lanes >= nl - nb, edge_i, turn(D, nl - nb, 1))
    t = pltpu.roll(D, 1, 0)
    down_j = jnp.where(subs == 0, jnp.where(block == 0, y_low, turn(t, 1, 1)), t)
    t = pltpu.roll(D, SUB - 1, 0)
    edge_j = jnp.where(last_y, 0, D + y_high)
    up_j = jnp.where(
        subs == SUB - 1, jnp.where(block == nb - 1, edge_j, turn(t, nl - 1, 1)), t
    )
    eh_ref[0:SUB] = 8 * D + (down_i + up_i) + (down_j + up_j)
    above = i_scan(j_scan(zdn0[...] + jnp.where(lanes < nb, zdn2[...], 0)))
    above = above + i_scan(zdn1[...])[0:1]
    eh_ref[SUB : 2 * SUB] = jnp.where(last_z, -D, above)

    for here, copy in ends:
        @pl.when(here)
        def _():
            copy().wait_send()


def finish(step_ref, v_ref, eh_ref, out_hbm, out, sems):
    ni, nj, nk = out.shape
    nb = nj // SUB
    scale = step_ref[0] * (1.0 / 12.0)
    at_end = iota((SUB, nk), 1) == nk - 1
    E, EH = eh_ref[0:SUB], eh_ref[0:SUB] + eh_ref[SUB : 2 * SUB]
    pieces = sems.shape[0]
    depth = ni // pieces
    copies = []
    for p in range(pieces):
        for i in range(p * depth, (p + 1) * depth):
            for b in range(nb):
                v = i * nb + b
                rows = slice(b * SUB, (b + 1) * SUB)
                carry = jnp.where(at_end, EH[:, v : v + 1], E[:, v : v + 1])
                out[i, rows, :] = (v_ref[i, rows, :] + carry).astype(F32) * scale
        part = pl.ds(p * depth, depth)
        copy = pltpu.make_async_copy(out.at[part], out_hbm.at[part], sems.at[p])
        copy.start()
        copies.append(copy)
    for copy in copies:
        copy.wait()


def solution(mesh):
    sizes = tuple(mesh.shape[a] for a in ("gx", "gy", "gz"))
    nx, ny, nz = sizes

    def on_device(quant_codes, error_step):
        ni, nj, nk = quant_codes.shape
        nl = ni * nj // SUB
        vm = lambda *shape: pltpu.VMEM(shape, I32)
        dma = lambda n: pltpu.SemaphoreType.DMA((n,))
        scratch = [
            vm(ni, nj, nk), vm(ni, nj, nk),
            vm(nj, nk), vm(nx - 1, nj, nk), vm(nj, nk),
            vm(ni, nk), vm(SUB, nk), vm(ny - 1, ni, nk), vm(ny - 1, SUB, nk),
            vm(ni, nk), vm(SUB, nk), vm(ni, nk), vm(SUB, nk),
            *[vm(SUB, nl)] * 3, *[vm(nz - 1, SUB, nl)] * 3,
            *[vm(SUB, nl)] * 6,
            vm(nj, nk), vm(nj, nk), vm(ni, nk), vm(SUB, nk),
            vm(nj, nk), vm(nj, nk), vm(ni, nk), vm(ni, nk),
            *[vm(SUB, nl)] * 3,
            pltpu.SemaphoreType.DMA,
            dma(nx - 1), dma(nx - 1), *[dma(ny - 1)] * 4, *[dma(nz - 1)] * 6,
            dma(6), dma(6),
        ]
        any_space = pl.BlockSpec(memory_space=pl.ANY)
        vmem = pl.BlockSpec(memory_space=pltpu.VMEM)
        v, eh = pl.pallas_call(
            functools.partial(exchange, sizes),
            out_shape=(
                jax.ShapeDtypeStruct((ni, nj, nk), I32),
                jax.ShapeDtypeStruct((2 * SUB, nl), I32),
            ),
            in_specs=[any_space],
            out_specs=(vmem, vmem),
            scratch_shapes=scratch,
            compiler_params=pltpu.CompilerParams(
                collective_id=0, has_side_effects=True, vmem_limit_bytes=16 * 2**20
            ),
            name="exchange",
        )(quant_codes)
        return pl.pallas_call(
            finish,
            out_shape=jax.ShapeDtypeStruct((ni, nj, nk), F32),
            in_specs=[pl.BlockSpec(memory_space=pltpu.SMEM), vmem, vmem],
            out_specs=any_space,
            scratch_shapes=[pltpu.VMEM((ni, nj, nk), F32), dma(4)],
            compiler_params=pltpu.CompilerParams(vmem_limit_bytes=16 * 2**20),
            name="finish",
        )(error_step, v, eh)

    return jax.shard_map(
        on_device, mesh=mesh, in_specs=(P("gx", "gy", "gz"), P()),
        out_specs=P("gx", "gy", "gz"), check_vma=False,
    )
```

```python
import functools

import jax
import jax.numpy as jnp
from jax import lax
from jax.experimental import pallas as pl
from jax.experimental.pallas import tpu as pltpu
from jax.sharding import PartitionSpec as P

MESH = pl.DeviceIdType.MESH
I32 = jnp.int32
F32 = jnp.float32
SUB = 8
GRANT = 16 * 2**20


def iota(shape, dim):
    return lax.broadcasted_iota(I32, shape, dim)


def turn(x, by, dim):
    n = x.shape[dim]
    by = by % n
    if by == 0:
        return x
    if dim == 1 and n % 128 != 0:
        return jnp.concatenate([x[:, n - by :], x[:, : n - by]], 1)
    return pltpu.roll(x, by, dim)


def lane_scan(x):
    n = x.shape[1]
    tri = (iota((n, n), 0) <= iota((n, n), 1)).astype(F32)
    one, big = tri.astype(jnp.bfloat16), (tri * 256.0).astype(jnp.bfloat16)

    def times(part, m):
        return jnp.dot(part.astype(F32).astype(jnp.bfloat16), m, preferred_element_type=F32)

    low = times(x & 255, one) + times((x >> 8) & 255, big)
    high = times((x >> 16) & 255, one) + times(x >> 24, big)
    return low.astype(I32) + (high.astype(I32) << 16)


def row_scan(x):
    rows, n = x.shape
    s = iota((SUB, n), 0)
    out, carry = [], None
    for b in range(rows // SUB):
        v = x[b * SUB : (b + 1) * SUB]
        for d in (1, 2, 4):
            v = v + jnp.where(s >= d, pltpu.roll(v, d, 0), 0)
        if carry is not None:
            v = v + carry
        carry = jnp.broadcast_to(v[SUB - 1 : SUB], (SUB, n))
        out.append(v)
    return jnp.concatenate(out, 0) if len(out) > 1 else out[0]


def exchange(
    mesh_sizes, q_hbm, v_ref, eh_ref,
    q, scan, xs, xup, xdn, ys, yup, hy, ydn, lines, cup, cx, cy,
    z0, z2, z1, zup0, zup2, zup1, d0, d2, d1, zdn0, zdn2, zdn1,
    rx, ry, ryt, ax, hxc, by, hyc, za0, za2, za1,
    load_sem, xss, xrs, yss, yrs, css, crs, z0ss, z0rs, z2ss, z2rs, z1ss, z1rs, dss, drs, ready,
):
    nx, ny, nz = mesh_sizes
    ni, nj, nk = q.shape
    nb = nj // SUB
    nl = ni * nb
    X, Y, Z = (lax.axis_index(a) for a in ("gx", "gy", "gz"))
    place = {"gx": X, "gy": Y, "gz": Z}
    size = {"gx": nx, "gy": ny, "gz": nz}
    last_x, last_y, last_z = X == nx - 1, Y == ny - 1, Z == nz - 1

    load = pltpu.make_async_copy(q_hbm, q, load_sem)
    load.start()
    barrier = pltpu.get_barrier_semaphore()

    def greet(to, axis, sem):
        pl.semaphore_signal(sem, inc=1, device_id={axis: to}, device_id_type=MESH)

    @pl.when(Z > 0)
    def _():
        greet(Z - 1, "gz", barrier)

    @pl.when(Z < nz - 1)
    def _():
        greet(Z + 1, "gz", barrier)

    for dx in range(nx):
        for dy in range(ny):
            if dx or dy:
                pl.semaphore_signal(
                    barrier, inc=1, device_id_type=MESH,
                    device_id={"gx": lax.rem(X + dx, nx), "gy": lax.rem(Y + dy, ny)},
                )

    ends = []

    def hear(d):
        @pl.when(Z + d < nz)
        def _():
            pl.semaphore_wait(ready.at[d - 2], 1)

            if d < nz - 1:
                @pl.when(Z > 0)
                def _():
                    greet(Z - 1, "gz", ready.at[d - 1])

    def up(axis, src, slots, ssem, rsem, first=False):
        for d in range(1, size[axis]):
            if first and d >= 2:
                hear(d)

            def copy(d=d):
                return pltpu.make_async_remote_copy(
                    src_ref=src, dst_ref=slots.at[d - 1], send_sem=ssem.at[d - 1],
                    recv_sem=rsem.at[d - 1], device_id={axis: place[axis] + d},
                    device_id_type=MESH,
                )

            here = place[axis] + d < size[axis]

            @pl.when(here)
            def _():
                copy().start()

            ends.append((here, copy))

    def up_sum(axis, src, slots, ssem, rsem, total):
        total[...] = jnp.zeros_like(total)
        for d in range(1, size[axis]):
            @pl.when(place[axis] >= d)
            def _():
                pltpu.make_async_remote_copy(
                    src_ref=src, dst_ref=slots.at[d - 1], send_sem=ssem.at[d - 1],
                    recv_sem=rsem.at[d - 1], device_id={axis: place[axis]},
                    device_id_type=MESH,
                ).wait_recv()
                total[...] += slots[d - 1]

    def down_copy(axis, src, dst, n):
        return pltpu.make_async_remote_copy(
            src_ref=src, dst_ref=dst, send_sem=dss.at[n], recv_sem=drs.at[n],
            device_id={axis: place[axis] - 1}, device_id_type=MESH,
        )

    def down(axis, src, dst, n):
        here = place[axis] > 0

        @pl.when(here)
        def _():
            down_copy(axis, src, dst, n).start()

        ends.append((here, lambda: down_copy(axis, src, dst, n)))

    def down_wait(axis, src, dst, n):
        @pl.when(place[axis] < size[axis] - 1)
        def _():
            down_copy(axis, src, dst, n).wait_recv()

        @pl.when(place[axis] == size[axis] - 1)
        def _():
            dst[...] = jnp.zeros_like(dst)

    lanes = iota((SUB, nl), 1)
    subs = iota((SUB, nl), 0)

    load.wait()
    total = q[0]
    for i in range(1, ni):
        total = total + q[i]
    xs[...] = total
    for i in range(ni):
        ys[pl.ds(i, 1), :] = jnp.sum(q[i], axis=0, keepdims=True)
        hy[pl.ds(i, 1), :] = q[i, 0:1, :]
    sk = iota((SUB, nk), 0)
    lines[...] = jnp.where(
        sk == 0, jnp.sum(total, axis=0, keepdims=True),
        jnp.where(
            sk == 1, jnp.sum(q[0], axis=0, keepdims=True),
            jnp.where(sk == 2, total[0:1], 0),
        ),
    )
    beside_z = (Z > 0).astype(I32) + (Z < nz - 1).astype(I32)
    pl.semaphore_wait(barrier, nx * ny - 1 + beside_z)
    up("gx", xs, xup, xss, xrs)
    down("gx", q.at[0], xdn, 0)
    up("gy", ys, yup, yss, yrs)
    down("gy", hy, ydn, 1)

    corners = []
    for dx in range(-1, nx):
        for dy in range(-1, ny):
            if dx > 0 and dy > 0:
                slot = cup.at[(dx - 1) * (ny - 1) + dy - 1]
            elif dx == -1 and dy > 0:
                slot = cx.at[dy - 1]
            elif dx > 0 and dy == -1:
                slot = cy.at[dx - 1]
            else:
                continue
            corners.append((dx, dy, slot, len(corners)))

    def inside(x, y):
        return (x >= 0) & (x < nx) & (y >= 0) & (y < ny)

    def corner_copy(dx, dy, slot, n):
        return pltpu.make_async_remote_copy(
            src_ref=lines, dst_ref=slot, send_sem=css.at[n], recv_sem=crs.at[n],
            device_id={"gx": X + dx, "gy": Y + dy}, device_id_type=MESH,
        )

    for c in corners:
        here = inside(X + c[0], Y + c[1])

        @pl.when(here)
        def _(c=c):
            corner_copy(*c).start()

        ends.append((here, functools.partial(corner_copy, *c)))
    if nz > 2:
        @pl.when((Z > 0) & (Z < nz - 1))
        def _():
            greet(Z - 1, "gz", ready.at[0])

    step = 8

    def scan_block(g, _):
        rows = pl.ds(g * step, step)
        part = q[rows].reshape(step * nj, nk)
        scan[rows] = lane_scan(part).reshape(step, nj, nk)
        return 0

    lax.fori_loop(0, ni // step, scan_block, 0)

    a0 = jnp.zeros((SUB, nl), I32)
    b0 = jnp.zeros((SUB, nl), I32)
    for i in range(ni):
        for b in range(nb):
            rows = slice(b * SUB, (b + 1) * SUB)
            here = lanes == i * nb + b
            a0 = jnp.where(here, scan[i, rows, nk - 1 : nk], a0)
            b0 = jnp.where(here, q[i, rows, 0:1], b0)
    z0[...] = a0
    d0[...] = b0
    up("gz", z0, zup0, z0ss, z0rs, first=True)
    down("gz", d0, zdn0, 2)
    up_sum("gx", xs, xup, xss, xrs, rx)
    down_wait("gx", q.at[0], xdn, 0)
    rxv, hxv = rx[...], xdn[...]
    lx = lane_scan(jnp.concatenate([rxv, hxv], 0))
    a2 = jnp.zeros((SUB, nl), I32)
    b2 = jnp.zeros((SUB, nl), I32)
    for b in range(2 * nb):
        rows = slice(b * SUB, (b + 1) * SUB)
        a2 = jnp.where(lanes == b, lx[rows, nk - 1 : nk], a2)
        if b < nb:
            b2 = jnp.where(lanes == b, rxv[rows, 0:1], b2)
    z2[...] = a2
    d2[...] = b2
    up("gz", z2, zup2, z2ss, z2rs)
    down("gz", d2, zdn2, 3)
    ax[...] = row_scan(lx[:nj])
    hxc[...] = row_scan(lx[nj:])

    up_sum("gy", ys, yup, yss, yrs, ry)
    down_wait("gy", hy, ydn, 1)
    ryt[...] = jnp.zeros_like(ryt)
    for c in corners:
        row = 0 if c[0] > 0 and c[1] > 0 else 1 if c[1] > 0 else 2

        @pl.when(inside(X - c[0], Y - c[1]))
        def _(c=c, row=row):
            corner_copy(*c).wait_recv()
            ryt[...] += jnp.where(sk == row, c[2][...], 0)

    ryv, rytv = ry[...], ryt[...]
    ly = lane_scan(jnp.concatenate([ryv, ydn[...], rytv], 0))
    lyl, lyh, lyt = ly[:ni], ly[ni : 2 * ni], ly[2 * ni :]
    lyht = lyt[2:3]
    mine = (iota((ni, nl), 1) // nb) == iota((ni, nl), 0)
    first = (iota((1, nl), 1) // nb) == 0

    def along(column, extra):
        row = jnp.sum(jnp.where(mine, column, 0), axis=0, keepdims=True)
        return row + jnp.where(first, extra, 0)

    end = slice(nk - 1, nk)
    z1[...] = jnp.where(
        subs == 0, along(lyl[:, end], lyt[0:1, end]),
        jnp.where(
            subs == 1, along(lyh[:, end], lyht[0:1, end]),
            jnp.where(
                subs == 2, lyt[0:1, end], jnp.where(subs == 3, lyt[1:2, end], 0)
            ),
        ),
    )
    d1[...] = jnp.where(subs == 0, along(ryv[:, 0:1], rytv[0:1, 0:1]), 0)
    up("gz", z1, zup1, z1ss, z1rs)
    down("gz", d1, zdn1, 4)

    rows_i = iota((ni, nk), 0)
    by[...] = row_scan(lyl + jnp.where(rows_i == 0, lyt[0:1], 0))
    hyc[...] = row_scan(lyh + jnp.where(rows_i == 0, lyht[0:1], 0))
    jrow = iota((nj, nk), 0)
    klane = iota((nj, nk), 1)
    plane = ax[...]

    def field(i, before):
        inner = before + row_scan(scan[i])
        return inner, inner + plane + by[pl.ds(i, 1), :]

    def stencil(i, low, mid, high):
        down_j = jnp.where(jrow == 0, by[pl.ds(i, 1), :], turn(mid, 1, 0))
        edge_j = jnp.where(last_y, 0, mid + hyc[pl.ds(i, 1), :])
        up_j = jnp.where(jrow == nj - 1, edge_j, turn(mid, nj - 1, 0))
        down_k = jnp.where(klane == 0, 0, turn(mid, 1, 1))
        edge_k = jnp.where(last_z, 0, mid)
        up_k = jnp.where(klane == nk - 1, edge_k, turn(mid, nk - 1, 1))
        v_ref[i] = 6 * mid + (low + high) + (down_j + up_j) + (down_k + up_k)

    def sweep(i, state):
        low, mid, before = state
        inner, high = field(i + 1, before)
        stencil(i, low, mid, high)
        return mid, high, inner

    inner, mid = field(0, jnp.zeros((nj, nk), I32))
    low, mid, _ = lax.fori_loop(0, ni - 1, sweep, (plane + lyt[0:1], mid, inner))
    stencil(ni - 1, low, mid, jnp.where(last_x, 0, mid + hxc[...] + lyt[1:2]))

    up_sum("gz", z0, zup0, z0ss, z0rs, za0)
    up_sum("gz", z2, zup2, z2ss, z2rs, za2)
    down_wait("gz", d0, zdn0, 2)
    down_wait("gz", d2, zdn2, 3)
    up_sum("gz", z1, zup1, z1ss, z1rs, za1)
    down_wait("gz", d1, zdn1, 4)
    block = lax.rem(lanes, nb)

    def j_scan(w):
        for d in (1, 2, 4):
            w = w + jnp.where(subs >= d, pltpu.roll(w, d, 0), 0)
        whole = jnp.broadcast_to(w[SUB - 1 : SUB], w.shape)
        for d in range(1, nb):
            w = w + jnp.where(block >= d, turn(whole, d, 1), 0)
        return w

    def i_scan(w):
        d = nb
        while d < nl:
            w = w + jnp.where(lanes >= d, turn(w, d, 1), 0)
            d *= 2
        return w

    r2, r1 = za2[...], za1[...]
    y = i_scan(r1)
    y_low, y_high = y[0:1], y[1:2]
    corner, corner_high = r1[2:3], r1[3:4]
    D = i_scan(j_scan(za0[...] + jnp.where(lanes < nb, r2, 0))) + y_low
    xe = j_scan(r2)
    down_i = jnp.where(lanes < nb, xe + corner, turn(D, nb, 1))
    edge_i = jnp.where(last_x, 0, D + turn(xe, nl - 2 * nb, 1) + corner_high)
    up_i = jnp.where(lanes >= nl - nb, edge_i, turn(D, nl - nb, 1))
    t = pltpu.roll(D, 1, 0)
    down_j = jnp.where(subs == 0, jnp.where(block == 0, y_low, turn(t, 1, 1)), t)
    t = pltpu.roll(D, SUB - 1, 0)
    edge_j = jnp.where(last_y, 0, D + y_high)
    up_j = jnp.where(
        subs == SUB - 1, jnp.where(block == nb - 1, edge_j, turn(t, nl - 1, 1)), t
    )
    eh_ref[0:SUB] = 8 * D + (down_i + up_i) + (down_j + up_j)
    above = i_scan(j_scan(zdn0[...] + jnp.where(lanes < nb, zdn2[...], 0)))
    above = above + i_scan(zdn1[...])[0:1]
    eh_ref[SUB : 2 * SUB] = jnp.where(last_z, -D, above)

    for here, copy in ends:
        @pl.when(here)
        def _():
            copy().wait_send()


def finish(step_ref, v_ref, eh_ref, out_hbm, out, sems):
    ni, nj, nk = out.shape
    nb = nj // SUB
    scale = step_ref[0] * (1.0 / 12.0)
    at_end = iota((SUB, nk), 1) == nk - 1
    E, EH = eh_ref[0:SUB], eh_ref[0:SUB] + eh_ref[SUB : 2 * SUB]
    pieces = sems.shape[0]
    depth = ni // pieces
    copies = []
    for p in range(pieces):
        for i in range(p * depth, (p + 1) * depth):
            for b in range(nb):
                v = i * nb + b
                rows = slice(b * SUB, (b + 1) * SUB)
                carry = jnp.where(at_end, EH[:, v : v + 1], E[:, v : v + 1])
                out[i, rows, :] = (v_ref[i, rows, :] + carry).astype(F32) * scale
        part = pl.ds(p * depth, depth)
        copy = pltpu.make_async_copy(out.at[part], out_hbm.at[part], sems.at[p])
        copy.start()
        copies.append(copy)
    for copy in copies:
        copy.wait()


def solution(mesh):
    sizes = tuple(mesh.shape[a] for a in ("gx", "gy", "gz"))
    nx, ny, nz = sizes

    def on_device(quant_codes, error_step):
        ni, nj, nk = quant_codes.shape
        nl = ni * nj // SUB
        vm = lambda *shape: pltpu.VMEM(shape, I32)
        dma = lambda n: pltpu.SemaphoreType.DMA((n,))
        scratch = [
            vm(ni, nj, nk), vm(ni, nj, nk),
            vm(nj, nk), vm(nx - 1, nj, nk), vm(nj, nk),
            vm(ni, nk), vm(ny - 1, ni, nk), vm(ni, nk), vm(ni, nk),
            vm(SUB, nk), vm((nx - 1) * (ny - 1), SUB, nk),
            vm(ny - 1, SUB, nk), vm(nx - 1, SUB, nk),
            *[vm(SUB, nl)] * 3, *[vm(nz - 1, SUB, nl)] * 3,
            *[vm(SUB, nl)] * 6,
            vm(nj, nk), vm(ni, nk), vm(SUB, nk),
            vm(nj, nk), vm(nj, nk), vm(ni, nk), vm(ni, nk),
            *[vm(SUB, nl)] * 3,
            pltpu.SemaphoreType.DMA,
            dma(nx - 1), dma(nx - 1), dma(ny - 1), dma(ny - 1),
            dma(nx * ny - 1 + nx * ny), dma(nx * ny - 1 + nx * ny), *[dma(nz - 1)] * 6,
            dma(5), dma(5),
            pltpu.SemaphoreType.REGULAR((max(nz - 2, 1),)),
        ]
        any_space = pl.BlockSpec(memory_space=pl.ANY)
        hbm = pl.BlockSpec(memory_space=pltpu.HBM)
        vmem = pl.BlockSpec(memory_space=pltpu.VMEM)
        v, eh = pl.pallas_call(
            functools.partial(exchange, sizes),
            out_shape=(
                jax.ShapeDtypeStruct((ni, nj, nk), I32),
                jax.ShapeDtypeStruct((2 * SUB, nl), I32),
            ),
            in_specs=[hbm],
            out_specs=(vmem, vmem),
            scratch_shapes=scratch,
            compiler_params=pltpu.CompilerParams(
                collective_id=0, has_side_effects=True, vmem_limit_bytes=GRANT
            ),
            name="exchange",
        )(pltpu.with_memory_space_constraint(quant_codes, pltpu.HBM))
        return pl.pallas_call(
            finish,
            out_shape=jax.ShapeDtypeStruct((ni, nj, nk), F32),
            in_specs=[pl.BlockSpec(memory_space=pltpu.SMEM), vmem, vmem],
            out_specs=any_space,
            scratch_shapes=[pltpu.VMEM((ni, nj, nk), F32), dma(4)],
            compiler_params=pltpu.CompilerParams(vmem_limit_bytes=16 * 2**20),
            name="finish",
        )(error_step, v, eh)

    return jax.shard_map(
        on_device, mesh=mesh, in_specs=(P("gx", "gy", "gz"), P()),
        out_specs=P("gx", "gy", "gz"), check_vma=False,
    )
```

```python
import functools

import jax
import jax.numpy as jnp
from jax import lax
from jax.experimental import pallas as pl
from jax.experimental.pallas import tpu as pltpu
from jax.sharding import PartitionSpec as P

MESH = pl.DeviceIdType.MESH
I32 = jnp.int32
F32 = jnp.float32
SUB = 8
GRANT = 16 * 2**20
UNROLL = 4


def iota(shape, dim):
    return lax.broadcasted_iota(I32, shape, dim)


def turn(x, by, dim):
    n = x.shape[dim]
    by = by % n
    if by == 0:
        return x
    if dim == 1 and n % 128 != 0:
        return jnp.concatenate([x[:, n - by :], x[:, : n - by]], 1)
    return pltpu.roll(x, by, dim)


def lane_scan(x):
    n = x.shape[1]
    tri = (iota((n, n), 0) <= iota((n, n), 1)).astype(F32)
    one, big = tri.astype(jnp.bfloat16), (tri * 256.0).astype(jnp.bfloat16)

    def times(part, m):
        return jnp.dot(part.astype(F32).astype(jnp.bfloat16), m, preferred_element_type=F32)

    low = times(x & 255, one) + times((x >> 8) & 255, big)
    high = times((x >> 16) & 255, one) + times(x >> 24, big)
    return low.astype(I32) + (high.astype(I32) << 16)


def row_scan(x):
    rows, n = x.shape
    s = iota((SUB, n), 0)
    out, carry = [], None
    for b in range(rows // SUB):
        v = x[b * SUB : (b + 1) * SUB]
        for d in (1, 2, 4):
            v = v + jnp.where(s >= d, pltpu.roll(v, d, 0), 0)
        if carry is not None:
            v = v + carry
        carry = jnp.broadcast_to(v[SUB - 1 : SUB], (SUB, n))
        out.append(v)
    return jnp.concatenate(out, 0) if len(out) > 1 else out[0]


def exchange(
    mesh_sizes, q_hbm, v_ref, eh_ref,
    q, scan, xs, xup, xdn, ys, yup, hy, ydn, lines, cup, cx, cy,
    zs, zup, ds, zdn, rx, ry, ryt, ax, hxc, by, hyc, carry,
    load_sem, xss, xrs, yss, yrs, css, crs, zss, zrs, dss, drs, ready,
):
    nx, ny, nz = mesh_sizes
    ni, nj, nk = q.shape
    nb = nj // SUB
    nl = ni * nb
    X, Y, Z = (lax.axis_index(a) for a in ("gx", "gy", "gz"))
    place = {"gx": X, "gy": Y, "gz": Z}
    size = {"gx": nx, "gy": ny, "gz": nz}
    last_x, last_y, last_z = X == nx - 1, Y == ny - 1, Z == nz - 1

    load = pltpu.make_async_copy(q_hbm, q, load_sem)
    load.start()
    barrier = pltpu.get_barrier_semaphore()

    def greet(to, axis, sem):
        pl.semaphore_signal(sem, inc=1, device_id={axis: to}, device_id_type=MESH)

    @pl.when(Z > 0)
    def _():
        greet(Z - 1, "gz", barrier)

    @pl.when(Z < nz - 1)
    def _():
        greet(Z + 1, "gz", barrier)

    for dx in range(nx):
        for dy in range(ny):
            if dx or dy:
                pl.semaphore_signal(
                    barrier, inc=1, device_id_type=MESH,
                    device_id={"gx": lax.rem(X + dx, nx), "gy": lax.rem(Y + dy, ny)},
                )

    ends = []

    def hear(d):
        @pl.when(Z + d < nz)
        def _():
            pl.semaphore_wait(ready.at[d - 2], 1)

            if d < nz - 1:
                @pl.when(Z > 0)
                def _():
                    greet(Z - 1, "gz", ready.at[d - 1])

    def up(axis, src, slots, ssem, rsem, steps=None):
        for d in steps or range(1, size[axis]):
            def copy(d=d):
                return pltpu.make_async_remote_copy(
                    src_ref=src, dst_ref=slots.at[d - 1], send_sem=ssem.at[d - 1],
                    recv_sem=rsem.at[d - 1], device_id={axis: place[axis] + d},
                    device_id_type=MESH,
                )

            here = place[axis] + d < size[axis]

            @pl.when(here)
            def _():
                copy().start()

            ends.append((here, copy))

    def up_sum(axis, src, slots, ssem, rsem, total):
        total[...] = jnp.zeros_like(total)
        for d in range(1, size[axis]):
            @pl.when(place[axis] >= d)
            def _():
                pltpu.make_async_remote_copy(
                    src_ref=src, dst_ref=slots.at[d - 1], send_sem=ssem.at[d - 1],
                    recv_sem=rsem.at[d - 1], device_id={axis: place[axis]},
                    device_id_type=MESH,
                ).wait_recv()
                total[...] += slots[d - 1]

    def down_copy(axis, src, dst, n):
        return pltpu.make_async_remote_copy(
            src_ref=src, dst_ref=dst, send_sem=dss.at[n], recv_sem=drs.at[n],
            device_id={axis: place[axis] - 1}, device_id_type=MESH,
        )

    def down(axis, src, dst, n):
        here = place[axis] > 0

        @pl.when(here)
        def _():
            down_copy(axis, src, dst, n).start()

        ends.append((here, lambda: down_copy(axis, src, dst, n)))

    def down_wait(axis, src, dst, n):
        @pl.when(place[axis] < size[axis] - 1)
        def _():
            down_copy(axis, src, dst, n).wait_recv()

        @pl.when(place[axis] == size[axis] - 1)
        def _():
            dst[...] = jnp.zeros_like(dst)

    lanes = iota((SUB, nl), 1)
    subs = iota((SUB, nl), 0)

    load.wait()
    total = q[0]
    for i in range(1, ni):
        total = total + q[i]
    xs[...] = total
    for i in range(ni):
        ys[pl.ds(i, 1), :] = jnp.sum(q[i], axis=0, keepdims=True)
        hy[pl.ds(i, 1), :] = q[i, 0:1, :]
    sk = iota((SUB, nk), 0)
    lines[...] = jnp.where(
        sk == 0, jnp.sum(total, axis=0, keepdims=True),
        jnp.where(
            sk == 1, jnp.sum(q[0], axis=0, keepdims=True),
            jnp.where(sk == 2, total[0:1], 0),
        ),
    )
    beside_z = (Z > 0).astype(I32) + (Z < nz - 1).astype(I32)
    pl.semaphore_wait(barrier, nx * ny - 1 + beside_z)
    down("gy", hy, ydn, 1)
    up("gy", ys, yup, yss, yrs)

    corners = []
    for dx in range(-1, nx):
        for dy in range(-1, ny):
            if dx > 0 and dy > 0:
                slot = cup.at[(dx - 1) * (ny - 1) + dy - 1]
            elif dx == -1 and dy > 0:
                slot = cx.at[dy - 1]
            elif dx > 0 and dy == -1:
                slot = cy.at[dx - 1]
            else:
                continue
            corners.append((dx, dy, slot, len(corners)))

    def inside(x, y):
        return (x >= 0) & (x < nx) & (y >= 0) & (y < ny)

    def corner_copy(dx, dy, slot, n):
        return pltpu.make_async_remote_copy(
            src_ref=lines, dst_ref=slot, send_sem=css.at[n], recv_sem=crs.at[n],
            device_id={"gx": X + dx, "gy": Y + dy}, device_id_type=MESH,
        )

    for c in corners:
        here = inside(X + c[0], Y + c[1])

        @pl.when(here)
        def _(c=c):
            corner_copy(*c).start()

        ends.append((here, functools.partial(corner_copy, *c)))
    up("gx", xs, xup, xss, xrs)
    down("gx", q.at[0], xdn, 0)
    if nz > 2:
        @pl.when((Z > 0) & (Z < nz - 1))
        def _():
            greet(Z - 1, "gz", ready.at[0])

    step = 8

    def scan_block(g, _):
        rows = pl.ds(g * step, step)
        part = q[rows].reshape(step * nj, nk)
        scan[rows] = lane_scan(part).reshape(step, nj, nk)
        return 0

    lax.fori_loop(0, ni // step, scan_block, 0)

    block = lax.rem(lanes, nb)

    def j_scan(w):
        for d in (1, 2, 4):
            w = w + jnp.where(subs >= d, pltpu.roll(w, d, 0), 0)
        whole = jnp.broadcast_to(w[SUB - 1 : SUB], w.shape)
        for d in range(1, nb):
            w = w + jnp.where(block >= d, turn(whole, d, 1), 0)
        return w

    def i_scan(w):
        d = nb
        while d < nl:
            w = w + jnp.where(lanes >= d, turn(w, d, 1), 0)
            d *= 2
        return w

    a0 = jnp.zeros((SUB, nl), I32)
    b0 = jnp.zeros((SUB, nl), I32)
    for i in range(ni):
        for b in range(nb):
            rows = slice(b * SUB, (b + 1) * SUB)
            here = lanes == i * nb + b
            a0 = jnp.where(here, scan[i, rows, nk - 1 : nk], a0)
            b0 = jnp.where(here, q[i, rows, 0:1], b0)
    up_sum("gx", xs, xup, xss, xrs, rx)
    down_wait("gx", q.at[0], xdn, 0)
    rxv, hxv = rx[...], xdn[...]
    lx = lane_scan(jnp.concatenate([rxv, hxv], 0))
    a2 = jnp.zeros((SUB, nl), I32)
    b2 = jnp.zeros((SUB, nl), I32)
    for b in range(2 * nb):
        rows = slice(b * SUB, (b + 1) * SUB)
        a2 = jnp.where(lanes == b, lx[rows, nk - 1 : nk], a2)
        if b < nb:
            b2 = jnp.where(lanes == b, rxv[rows, 0:1], b2)
    a0 = i_scan(j_scan(a0 + jnp.where(lanes < nb, a2, 0)))
    b0 = i_scan(j_scan(b0 + jnp.where(lanes < nb, b2, 0)))
    a2 = j_scan(a2)
    for d in range(2, nz):
        @pl.when(Z > 0)
        def _(d=d):
            hear(d)

    ax[...] = row_scan(lx[:nj])
    hxc[...] = row_scan(lx[nj:])

    up_sum("gy", ys, yup, yss, yrs, ry)
    down_wait("gy", hy, ydn, 1)
    ryt[...] = jnp.zeros_like(ryt)
    for c in corners:
        row = 0 if c[0] > 0 and c[1] > 0 else 1 if c[1] > 0 else 2

        @pl.when(inside(X - c[0], Y - c[1]))
        def _(c=c, row=row):
            corner_copy(*c).wait_recv()
            ryt[...] += jnp.where(sk == row, c[2][...], 0)

    ryv, rytv = ry[...], ryt[...]
    ly = lane_scan(jnp.concatenate([ryv, ydn[...], rytv], 0))
    lyl, lyh, lyt = ly[:ni], ly[ni : 2 * ni], ly[2 * ni :]
    lyht = lyt[2:3]
    upto = (iota((ni, nl), 1) // nb) >= iota((ni, nl), 0)

    def along(column, extra):
        return jnp.sum(jnp.where(upto, column, 0), axis=0, keepdims=True) + extra

    end = slice(nk - 1, nk)
    y_low = along(lyl[:, end], lyt[0:1, end])
    y_high = along(lyh[:, end], lyht[0:1, end])
    zs[0:SUB] = a0 + y_low
    zs[SUB : 2 * SUB] = a2 + jnp.where(lanes < nb, lyt[0:1, end], lyt[1:2, end])
    zs[2 * SUB :] = jnp.where(subs == 0, y_low, jnp.where(subs == 1, y_high, 0))
    ds[...] = b0 + along(ryv[:, 0:1], rytv[0:1, 0:1])
    down("gz", ds, zdn, 2)
    up("gz", zs, zup, zss, zrs, [1])

    rows_i = iota((ni, nk), 0)
    by[...] = row_scan(lyl + jnp.where(rows_i == 0, lyt[0:1], 0))
    hyc[...] = row_scan(lyh + jnp.where(rows_i == 0, lyht[0:1], 0))
    jrow = iota((nj, nk), 0)
    klane = iota((nj, nk), 1)
    plane = ax[...]

    def field(i, before):
        inner = before + row_scan(scan[i])
        return inner, inner + plane + by[pl.ds(i, 1), :]

    def stencil(i, low, mid, high):
        down_j = jnp.where(jrow == 0, by[pl.ds(i, 1), :], turn(mid, 1, 0))
        edge_j = jnp.where(last_y, 0, mid + hyc[pl.ds(i, 1), :])
        up_j = jnp.where(jrow == nj - 1, edge_j, turn(mid, nj - 1, 0))
        down_k = jnp.where(klane == 0, 0, turn(mid, 1, 1))
        edge_k = jnp.where(last_z, 0, mid)
        up_k = jnp.where(klane == nk - 1, edge_k, turn(mid, nk - 1, 1))
        v_ref[i] = 6 * mid + (low + high) + (down_j + up_j) + (down_k + up_k)

    def sweep(i, state):
        low, mid, before = state
        inner, high = field(i + 1, before)
        stencil(i, low, mid, high)
        return mid, high, inner

    inner, mid = field(0, jnp.zeros((nj, nk), I32))
    state = (plane + lyt[0:1], mid, inner)
    many = (ni - 1) // UNROLL

    def sweeps(g, state):
        for u in range(UNROLL):
            state = sweep(g * UNROLL + u, state)
        return state

    state = lax.fori_loop(0, many, sweeps, state)
    for i in range(many * UNROLL, ni - 1):
        state = sweep(i, state)
    low, mid, _ = state
    stencil(ni - 1, low, mid, jnp.where(last_x, 0, mid + hxc[...] + lyt[1:2]))

    for d in range(2, nz):
        @pl.when(Z == 0)
        def _(d=d):
            hear(d)

        up("gz", zs, zup, zss, zrs, [d])

    up_sum("gz", zs, zup, zss, zrs, carry)
    down_wait("gz", ds, zdn, 2)
    D, xe = carry[0:SUB], carry[SUB : 2 * SUB]
    y_low, y_high = carry[2 * SUB : 2 * SUB + 1], carry[2 * SUB + 1 : 2 * SUB + 2]
    down_i = jnp.where(lanes < nb, xe, turn(D, nb, 1))
    edge_i = jnp.where(last_x, 0, D + turn(xe, nl - 2 * nb, 1))
    up_i = jnp.where(lanes >= nl - nb, edge_i, turn(D, nl - nb, 1))
    t = pltpu.roll(D, 1, 0)
    down_j = jnp.where(subs == 0, jnp.where(block == 0, y_low, turn(t, 1, 1)), t)
    t = pltpu.roll(D, SUB - 1, 0)
    edge_j = jnp.where(last_y, 0, D + y_high)
    up_j = jnp.where(
        subs == SUB - 1, jnp.where(block == nb - 1, edge_j, turn(t, nl - 1, 1)), t
    )
    eh_ref[0:SUB] = 8 * D + (down_i + up_i) + (down_j + up_j)
    eh_ref[SUB : 2 * SUB] = jnp.where(last_z, -D, zdn[...])

    for here, copy in ends:
        @pl.when(here)
        def _():
            copy().wait_send()


def finish(step_ref, v_ref, eh_ref, out_hbm, out, sems):
    ni, nj, nk = out.shape
    nb = nj // SUB
    scale = step_ref[0] * (1.0 / 12.0)
    at_end = iota((SUB, nk), 1) == nk - 1
    E, EH = eh_ref[0:SUB], eh_ref[0:SUB] + eh_ref[SUB : 2 * SUB]
    pieces = sems.shape[0]
    depth = ni // pieces
    copies = []
    for p in range(pieces):
        for i in range(p * depth, (p + 1) * depth):
            for b in range(nb):
                v = i * nb + b
                rows = slice(b * SUB, (b + 1) * SUB)
                carry = jnp.where(at_end, EH[:, v : v + 1], E[:, v : v + 1])
                out[i, rows, :] = (v_ref[i, rows, :] + carry).astype(F32) * scale
        part = pl.ds(p * depth, depth)
        copy = pltpu.make_async_copy(out.at[part], out_hbm.at[part], sems.at[p])
        copy.start()
        copies.append(copy)
    for copy in copies:
        copy.wait()


def solution(mesh):
    sizes = tuple(mesh.shape[a] for a in ("gx", "gy", "gz"))
    nx, ny, nz = sizes

    def on_device(quant_codes, error_step):
        ni, nj, nk = quant_codes.shape
        nl = ni * nj // SUB
        vm = lambda *shape: pltpu.VMEM(shape, I32)
        dma = lambda n: pltpu.SemaphoreType.DMA((n,))
        scratch = [
            vm(ni, nj, nk), vm(ni, nj, nk),
            vm(nj, nk), vm(nx - 1, nj, nk), vm(nj, nk),
            vm(ni, nk), vm(ny - 1, ni, nk), vm(ni, nk), vm(ni, nk),
            vm(SUB, nk), vm((nx - 1) * (ny - 1), SUB, nk),
            vm(ny - 1, SUB, nk), vm(nx - 1, SUB, nk),
            vm(3 * SUB, nl), vm(nz - 1, 3 * SUB, nl), vm(SUB, nl), vm(SUB, nl),
            vm(nj, nk), vm(ni, nk), vm(SUB, nk),
            vm(nj, nk), vm(nj, nk), vm(ni, nk), vm(ni, nk),
            vm(3 * SUB, nl),
            pltpu.SemaphoreType.DMA,
            dma(nx - 1), dma(nx - 1), dma(ny - 1), dma(ny - 1),
            dma(nx * ny - 1 + nx * ny), dma(nx * ny - 1 + nx * ny), dma(nz - 1), dma(nz - 1),
            dma(3), dma(3),
            pltpu.SemaphoreType.REGULAR((max(nz - 2, 1),)),
        ]
        any_space = pl.BlockSpec(memory_space=pl.ANY)
        hbm = pl.BlockSpec(memory_space=pltpu.HBM)
        vmem = pl.BlockSpec(memory_space=pltpu.VMEM)
        v, eh = pl.pallas_call(
            functools.partial(exchange, sizes),
            out_shape=(
                jax.ShapeDtypeStruct((ni, nj, nk), I32),
                jax.ShapeDtypeStruct((2 * SUB, nl), I32),
            ),
            in_specs=[hbm],
            out_specs=(vmem, vmem),
            scratch_shapes=scratch,
            compiler_params=pltpu.CompilerParams(
                collective_id=0, has_side_effects=True, vmem_limit_bytes=GRANT
            ),
            name="exchange",
        )(pltpu.with_memory_space_constraint(quant_codes, pltpu.HBM))
        return pl.pallas_call(
            finish,
            out_shape=jax.ShapeDtypeStruct((ni, nj, nk), F32),
            in_specs=[pl.BlockSpec(memory_space=pltpu.SMEM), vmem, vmem],
            out_specs=any_space,
            scratch_shapes=[pltpu.VMEM((ni, nj, nk), F32), dma(4)],
            compiler_params=pltpu.CompilerParams(vmem_limit_bytes=16 * 2**20),
            name="finish",
        )(error_step, v, eh)

    return jax.shard_map(
        on_device, mesh=mesh, in_specs=(P("gx", "gy", "gz"), P()),
        out_specs=P("gx", "gy", "gz"), check_vma=False,
    )
```

```python
import functools

import jax
import jax.numpy as jnp
from jax import lax
from jax.experimental import pallas as pl
from jax.experimental.pallas import tpu as pltpu
from jax.sharding import PartitionSpec as P

MESH = pl.DeviceIdType.MESH
I32 = jnp.int32
F32 = jnp.float32
SUB = 8
GRANT = 16 * 2**20
UNROLL = 4


def iota(shape, dim):
    return lax.broadcasted_iota(I32, shape, dim)


def turn(x, by, dim):
    n = x.shape[dim]
    by = by % n
    if by == 0:
        return x
    if dim == 1 and n % 128 != 0:
        return jnp.concatenate([x[:, n - by :], x[:, : n - by]], 1)
    return pltpu.roll(x, by, dim)


def lane_scan(x):
    n = x.shape[1]
    tri = (iota((n, n), 0) <= iota((n, n), 1)).astype(F32)
    one, big = tri.astype(jnp.bfloat16), (tri * 256.0).astype(jnp.bfloat16)

    def times(part, m):
        return jnp.dot(part.astype(F32).astype(jnp.bfloat16), m, preferred_element_type=F32)

    low = times(x & 255, one) + times((x >> 8) & 255, big)
    high = times((x >> 16) & 255, one) + times(x >> 24, big)
    return low.astype(I32) + (high.astype(I32) << 16)


def row_scan(x):
    rows, n = x.shape
    s = iota((SUB, n), 0)
    out, carry = [], None
    for b in range(rows // SUB):
        v = x[b * SUB : (b + 1) * SUB]
        for d in (1, 2, 4):
            v = v + jnp.where(s >= d, pltpu.roll(v, d, 0), 0)
        if carry is not None:
            v = v + carry
        carry = jnp.broadcast_to(v[SUB - 1 : SUB], (SUB, n))
        out.append(v)
    return jnp.concatenate(out, 0) if len(out) > 1 else out[0]


def exchange(
    mesh_sizes, q_hbm, v_ref, eh_ref,
    q, scan, xs, xup, xdn, ys, yup, hy, ydn, lines, cup, cx, cy,
    zs, zup, ds, zdn, rx, ry, ryt, ax, hxc, by, hyc, carry,
    load_sem, xss, xrs, yss, yrs, css, crs, zss, zrs, dss, drs, ready,
):
    nx, ny, nz = mesh_sizes
    ni, nj, nk = q.shape
    nb = nj // SUB
    nl = ni * nb
    X, Y, Z = (lax.axis_index(a) for a in ("gx", "gy", "gz"))
    place = {"gx": X, "gy": Y, "gz": Z}
    size = {"gx": nx, "gy": ny, "gz": nz}
    last_x, last_y, last_z = X == nx - 1, Y == ny - 1, Z == nz - 1

    load = pltpu.make_async_copy(q_hbm, q, load_sem)
    load.start()
    barrier = pltpu.get_barrier_semaphore()

    def greet(to, axis, sem):
        pl.semaphore_signal(sem, inc=1, device_id={axis: to}, device_id_type=MESH)

    @pl.when(Z > 0)
    def _():
        greet(Z - 1, "gz", barrier)

    @pl.when(Z < nz - 1)
    def _():
        greet(Z + 1, "gz", barrier)

    for dx in range(nx):
        for dy in range(ny):
            if dx or dy:
                pl.semaphore_signal(
                    barrier, inc=1, device_id_type=MESH,
                    device_id={"gx": lax.rem(X + dx, nx), "gy": lax.rem(Y + dy, ny)},
                )

    ends = []

    def hear(d):
        @pl.when(Z + d < nz)
        def _():
            pl.semaphore_wait(ready.at[d - 2], 1)

            if d < nz - 1:
                @pl.when(Z > 0)
                def _():
                    greet(Z - 1, "gz", ready.at[d - 1])

    def up(axis, src, slots, ssem, rsem, steps=None):
        for d in steps or range(1, size[axis]):
            def copy(d=d):
                return pltpu.make_async_remote_copy(
                    src_ref=src, dst_ref=slots.at[d - 1], send_sem=ssem.at[d - 1],
                    recv_sem=rsem.at[d - 1], device_id={axis: place[axis] + d},
                    device_id_type=MESH,
                )

            here = place[axis] + d < size[axis]

            @pl.when(here)
            def _():
                copy().start()

            ends.append((here, copy))

    def up_sum(axis, src, slots, ssem, rsem, total):
        total[...] = jnp.zeros_like(total)
        for d in range(1, size[axis]):
            @pl.when(place[axis] >= d)
            def _():
                pltpu.make_async_remote_copy(
                    src_ref=src, dst_ref=slots.at[d - 1], send_sem=ssem.at[d - 1],
                    recv_sem=rsem.at[d - 1], device_id={axis: place[axis]},
                    device_id_type=MESH,
                ).wait_recv()
                total[...] += slots[d - 1]

    def down_copy(axis, src, dst, n):
        return pltpu.make_async_remote_copy(
            src_ref=src, dst_ref=dst, send_sem=dss.at[n], recv_sem=drs.at[n],
            device_id={axis: place[axis] - 1}, device_id_type=MESH,
        )

    def down(axis, src, dst, n):
        here = place[axis] > 0

        @pl.when(here)
        def _():
            down_copy(axis, src, dst, n).start()

        ends.append((here, lambda: down_copy(axis, src, dst, n)))

    def down_wait(axis, src, dst, n):
        @pl.when(place[axis] < size[axis] - 1)
        def _():
            down_copy(axis, src, dst, n).wait_recv()

        @pl.when(place[axis] == size[axis] - 1)
        def _():
            dst[...] = jnp.zeros_like(dst)

    lanes = iota((SUB, nl), 1)
    subs = iota((SUB, nl), 0)

    load.wait()
    total = q[0]
    for i in range(1, ni):
        total = total + q[i]
    xs[...] = total
    for i in range(ni):
        ys[pl.ds(i, 1), :] = jnp.sum(q[i], axis=0, keepdims=True)
        hy[pl.ds(i, 1), :] = q[i, 0:1, :]
    sk = iota((SUB, nk), 0)
    lines[...] = jnp.where(
        sk == 0, jnp.sum(total, axis=0, keepdims=True),
        jnp.where(
            sk == 1, jnp.sum(q[0], axis=0, keepdims=True),
            jnp.where(sk == 2, total[0:1], 0),
        ),
    )
    beside_z = (Z > 0).astype(I32) + (Z < nz - 1).astype(I32)
    pl.semaphore_wait(barrier, nx * ny - 1 + beside_z)
    down("gy", hy, ydn, 1)
    up("gy", ys, yup, yss, yrs)

    corners = []
    for dx in range(-1, nx):
        for dy in range(-1, ny):
            if dx > 0 and dy > 0:
                slot = cup.at[(dx - 1) * (ny - 1) + dy - 1]
            elif dx == -1 and dy > 0:
                slot = cx.at[dy - 1]
            elif dx > 0 and dy == -1:
                slot = cy.at[dx - 1]
            else:
                continue
            corners.append((dx, dy, slot, len(corners)))

    def inside(x, y):
        return (x >= 0) & (x < nx) & (y >= 0) & (y < ny)

    def corner_copy(dx, dy, slot, n):
        return pltpu.make_async_remote_copy(
            src_ref=lines, dst_ref=slot, send_sem=css.at[n], recv_sem=crs.at[n],
            device_id={"gx": X + dx, "gy": Y + dy}, device_id_type=MESH,
        )

    for c in corners:
        here = inside(X + c[0], Y + c[1])

        @pl.when(here)
        def _(c=c):
            corner_copy(*c).start()

        ends.append((here, functools.partial(corner_copy, *c)))
    up("gx", xs, xup, xss, xrs)
    down("gx", q.at[0], xdn, 0)
    if nz > 2:
        @pl.when((Z > 0) & (Z < nz - 1))
        def _():
            greet(Z - 1, "gz", ready.at[0])

    step = 8

    def scan_block(g, _):
        rows = pl.ds(g * step, step)
        part = q[rows].reshape(step * nj, nk)
        scan[rows] = lane_scan(part).reshape(step, nj, nk)
        return 0

    lax.fori_loop(0, ni // step, scan_block, 0)

    block = lax.rem(lanes, nb)

    def j_scan(w):
        for d in (1, 2, 4):
            w = w + jnp.where(subs >= d, pltpu.roll(w, d, 0), 0)
        whole = jnp.broadcast_to(w[SUB - 1 : SUB], w.shape)
        for d in range(1, nb):
            w = w + jnp.where(block >= d, turn(whole, d, 1), 0)
        return w

    def i_scan(w):
        d = nb
        while d < nl:
            w = w + jnp.where(lanes >= d, turn(w, d, 1), 0)
            d *= 2
        return w

    a0 = jnp.zeros((SUB, nl), I32)
    b0 = jnp.zeros((SUB, nl), I32)
    for i in range(ni):
        for b in range(nb):
            rows = slice(b * SUB, (b + 1) * SUB)
            here = lanes == i * nb + b
            a0 = jnp.where(here, scan[i, rows, nk - 1 : nk], a0)
            b0 = jnp.where(here, q[i, rows, 0:1], b0)
    up_sum("gx", xs, xup, xss, xrs, rx)
    down_wait("gx", q.at[0], xdn, 0)
    rxv, hxv = rx[...], xdn[...]
    lx = lane_scan(jnp.concatenate([rxv, hxv], 0))
    a2 = jnp.zeros((SUB, nl), I32)
    b2 = jnp.zeros((SUB, nl), I32)
    for b in range(2 * nb):
        rows = slice(b * SUB, (b + 1) * SUB)
        a2 = jnp.where(lanes == b, lx[rows, nk - 1 : nk], a2)
        if b < nb:
            b2 = jnp.where(lanes == b, rxv[rows, 0:1], b2)
    a0 = i_scan(j_scan(a0 + jnp.where(lanes < nb, a2, 0)))
    b0 = i_scan(j_scan(b0 + jnp.where(lanes < nb, b2, 0)))
    a2 = j_scan(a2)
    for d in range(2, nz):
        @pl.when(Z > 0)
        def _(d=d):
            hear(d)

    ax[...] = row_scan(lx[:nj])
    hxc[...] = row_scan(lx[nj:])

    up_sum("gy", ys, yup, yss, yrs, ry)
    ryt[...] = jnp.zeros_like(ryt)

    def gather_lines(wanted):
        for c in corners:
            row = 0 if c[0] > 0 and c[1] > 0 else 1 if c[1] > 0 else 2
            if (row == 0) != wanted:
                continue

            @pl.when(inside(X - c[0], Y - c[1]))
            def _(c=c, row=row):
                corner_copy(*c).wait_recv()
                ryt[...] += jnp.where(sk == row, c[2][...], 0)

    upto = (iota((ni, nl), 1) // nb) >= iota((ni, nl), 0)

    def along(column, extra):
        return jnp.sum(jnp.where(upto, column, 0), axis=0, keepdims=True) + extra

    gather_lines(True)
    ds[...] = b0 + along(ry[:, 0:1], ryt[0:1, 0:1])
    down("gz", ds, zdn, 2)
    down_wait("gy", hy, ydn, 1)
    gather_lines(False)
    ryv, rytv = ry[...], ryt[...]
    ly = lane_scan(jnp.concatenate([ryv, ydn[...], rytv], 0))
    lyl, lyh, lyt = ly[:ni], ly[ni : 2 * ni], ly[2 * ni :]
    lyht = lyt[2:3]
    end = slice(nk - 1, nk)
    y_low = along(lyl[:, end], lyt[0:1, end])
    y_high = along(lyh[:, end], lyht[0:1, end])
    zs[0:SUB] = a0 + y_low
    zs[SUB : 2 * SUB] = a2 + jnp.where(lanes < nb, lyt[0:1, end], lyt[1:2, end])
    zs[2 * SUB :] = jnp.where(subs == 0, y_low, jnp.where(subs == 1, y_high, 0))
    up("gz", zs, zup, zss, zrs, [1])

    rows_i = iota((ni, nk), 0)
    by[...] = row_scan(lyl + jnp.where(rows_i == 0, lyt[0:1], 0))
    hyc[...] = row_scan(lyh + jnp.where(rows_i == 0, lyht[0:1], 0))
    jrow = iota((nj, nk), 0)
    klane = iota((nj, nk), 1)
    plane = ax[...]

    def field(i, before):
        inner = before + row_scan(scan[i])
        return inner, inner + plane + by[pl.ds(i, 1), :]

    def stencil(i, low, mid, high):
        down_j = jnp.where(jrow == 0, by[pl.ds(i, 1), :], turn(mid, 1, 0))
        edge_j = jnp.where(last_y, 0, mid + hyc[pl.ds(i, 1), :])
        up_j = jnp.where(jrow == nj - 1, edge_j, turn(mid, nj - 1, 0))
        down_k = jnp.where(klane == 0, 0, turn(mid, 1, 1))
        edge_k = jnp.where(last_z, 0, mid)
        up_k = jnp.where(klane == nk - 1, edge_k, turn(mid, nk - 1, 1))
        v_ref[i] = 6 * mid + (low + high) + (down_j + up_j) + (down_k + up_k)

    def sweep(i, state):
        low, mid, before = state
        inner, high = field(i + 1, before)
        stencil(i, low, mid, high)
        return mid, high, inner

    inner, mid = field(0, jnp.zeros((nj, nk), I32))
    state = (plane + lyt[0:1], mid, inner)
    many = (ni - 1) // UNROLL

    def sweeps(g, state):
        for u in range(UNROLL):
            state = sweep(g * UNROLL + u, state)
        return state

    state = lax.fori_loop(0, many, sweeps, state)
    for i in range(many * UNROLL, ni - 1):
        state = sweep(i, state)
    low, mid, _ = state
    stencil(ni - 1, low, mid, jnp.where(last_x, 0, mid + hxc[...] + lyt[1:2]))

    for d in range(2, nz):
        @pl.when(Z == 0)
        def _(d=d):
            hear(d)

        up("gz", zs, zup, zss, zrs, [d])

    up_sum("gz", zs, zup, zss, zrs, carry)
    down_wait("gz", ds, zdn, 2)
    D, xe = carry[0:SUB], carry[SUB : 2 * SUB]
    y_low, y_high = carry[2 * SUB : 2 * SUB + 1], carry[2 * SUB + 1 : 2 * SUB + 2]
    down_i = jnp.where(lanes < nb, xe, turn(D, nb, 1))
    edge_i = jnp.where(last_x, 0, D + turn(xe, nl - 2 * nb, 1))
    up_i = jnp.where(lanes >= nl - nb, edge_i, turn(D, nl - nb, 1))
    t = pltpu.roll(D, 1, 0)
    down_j = jnp.where(subs == 0, jnp.where(block == 0, y_low, turn(t, 1, 1)), t)
    t = pltpu.roll(D, SUB - 1, 0)
    edge_j = jnp.where(last_y, 0, D + y_high)
    up_j = jnp.where(
        subs == SUB - 1, jnp.where(block == nb - 1, edge_j, turn(t, nl - 1, 1)), t
    )
    eh_ref[0:SUB] = 8 * D + (down_i + up_i) + (down_j + up_j)
    eh_ref[SUB : 2 * SUB] = jnp.where(last_z, -D, zdn[...])

    for here, copy in ends:
        @pl.when(here)
        def _():
            copy().wait_send()


def finish(step_ref, v_ref, eh_ref, out_hbm, out, sems):
    ni, nj, nk = out.shape
    nb = nj // SUB
    scale = step_ref[0] * (1.0 / 12.0)
    at_end = iota((SUB, nk), 1) == nk - 1
    E, EH = eh_ref[0:SUB], eh_ref[0:SUB] + eh_ref[SUB : 2 * SUB]
    pieces = sems.shape[0]
    depth = ni // pieces
    copies = []
    for p in range(pieces):
        for i in range(p * depth, (p + 1) * depth):
            for b in range(nb):
                v = i * nb + b
                rows = slice(b * SUB, (b + 1) * SUB)
                carry = jnp.where(at_end, EH[:, v : v + 1], E[:, v : v + 1])
                out[i, rows, :] = (v_ref[i, rows, :] + carry).astype(F32) * scale
        part = pl.ds(p * depth, depth)
        copy = pltpu.make_async_copy(out.at[part], out_hbm.at[part], sems.at[p])
        copy.start()
        copies.append(copy)
    for copy in copies:
        copy.wait()


def solution(mesh):
    sizes = tuple(mesh.shape[a] for a in ("gx", "gy", "gz"))
    nx, ny, nz = sizes

    def on_device(quant_codes, error_step):
        ni, nj, nk = quant_codes.shape
        nl = ni * nj // SUB
        vm = lambda *shape: pltpu.VMEM(shape, I32)
        dma = lambda n: pltpu.SemaphoreType.DMA((n,))
        scratch = [
            vm(ni, nj, nk), vm(ni, nj, nk),
            vm(nj, nk), vm(nx - 1, nj, nk), vm(nj, nk),
            vm(ni, nk), vm(ny - 1, ni, nk), vm(ni, nk), vm(ni, nk),
            vm(SUB, nk), vm((nx - 1) * (ny - 1), SUB, nk),
            vm(ny - 1, SUB, nk), vm(nx - 1, SUB, nk),
            vm(3 * SUB, nl), vm(nz - 1, 3 * SUB, nl), vm(SUB, nl), vm(SUB, nl),
            vm(nj, nk), vm(ni, nk), vm(SUB, nk),
            vm(nj, nk), vm(nj, nk), vm(ni, nk), vm(ni, nk),
            vm(3 * SUB, nl),
            pltpu.SemaphoreType.DMA,
            dma(nx - 1), dma(nx - 1), dma(ny - 1), dma(ny - 1),
            dma(nx * ny - 1 + nx * ny), dma(nx * ny - 1 + nx * ny), dma(nz - 1), dma(nz - 1),
            dma(3), dma(3),
            pltpu.SemaphoreType.REGULAR((max(nz - 2, 1),)),
        ]
        any_space = pl.BlockSpec(memory_space=pl.ANY)
        hbm = pl.BlockSpec(memory_space=pltpu.HBM)
        vmem = pl.BlockSpec(memory_space=pltpu.VMEM)
        v, eh = pl.pallas_call(
            functools.partial(exchange, sizes),
            out_shape=(
                jax.ShapeDtypeStruct((ni, nj, nk), I32),
                jax.ShapeDtypeStruct((2 * SUB, nl), I32),
            ),
            in_specs=[hbm],
            out_specs=(vmem, vmem),
            scratch_shapes=scratch,
            compiler_params=pltpu.CompilerParams(
                collective_id=0, has_side_effects=True, vmem_limit_bytes=GRANT
            ),
            name="exchange",
        )(pltpu.with_memory_space_constraint(quant_codes, pltpu.HBM))
        return pl.pallas_call(
            finish,
            out_shape=jax.ShapeDtypeStruct((ni, nj, nk), F32),
            in_specs=[pl.BlockSpec(memory_space=pltpu.SMEM), vmem, vmem],
            out_specs=any_space,
            scratch_shapes=[pltpu.VMEM((ni, nj, nk), F32), dma(4)],
            compiler_params=pltpu.CompilerParams(vmem_limit_bytes=16 * 2**20),
            name="finish",
        )(error_step, v, eh)

    return jax.shard_map(
        on_device, mesh=mesh, in_specs=(P("gx", "gy", "gz"), P()),
        out_specs=P("gx", "gy", "gz"), check_vma=False,
    )
```
